256 devices in a mesh: wide: 16 (over y, x), narrow: 16 (over z, core).
Axes of the slice: x: 4, y: 4, z: 8, core: 2. Of those that a mesh axis runs over, the one named last changes fastest.
Arguments:
- vectors: float32 [524288, 128], P(('wide', 'narrow')), may hold values from -24 to 24
- near_blocks: bfloat16 [1024, 3, 512, 512], P(('wide', 'narrow')), may hold values from -0.15625 to 0.15625
- leaf_basis: bfloat16 [524288, 256], P(('wide', 'narrow')), may hold values from -0.125 to 0.125
- transfer: bfloat16 [256, 256, 256], P(('wide', 'narrow')), may hold values from -0.09375 to 0.09375
- leaf_coupling: bfloat16 [256, 6, 256, 256], P(('wide', 'narrow')), may hold values from -0.15625 to 0.15625
- leaf_partners: int32 [256, 6], P(('wide', 'narrow')), may hold values from 0 to 15, as said below
- parent_coupling: bfloat16 [16, 3, 256, 256], P('wide'), may hold values from -0.21875 to 0.21875
- parent_partners: int32 [16, 3], P('wide'), may hold values from 0 to 15, as said below
- shifts: float32 [128], replicated, may hold values from -1 to 1
Outputs:
- filtered: float32 [524288, 128], P(('wide', 'narrow'))
The draws below stay inside these ranges and needn't reach their ends.
Inputs may be any that keep to these rules, and one draw needn't show every extreme that they name: `leaf_partners`: row l lists 6 different sibling indices, none equal to l mod 16. `parent_partners`: row p lists 3 different parent indices, none equal to p.
All inputs are finite; a program needn't handle non-finite values.
Results may differ from the reference program's by a relative error of at most 0.01.
Values may be sent and summed in bfloat16 or wider, within the bound.
No kernel may reach another device: no remote copies, remote signals or barrier semaphores. Data moves between devices by JAX's collectives and lax.ppermute only.
A program may use at most 64 MiB of HBM per device.

```python
import jax
import jax.numpy as jnp
from jax import lax

NPTS_DEV = 2048
NVEC = 128
R = 256
BLK = 512
DEGREE = 3
K_LEAF = 6
K_TOP = 3
LEAVES = 256
NPTS = 524288
NBLK = 1024
BLOCKS_DEV = 4
N_WIDE = 16
N_NARROW = 16


def distinct_rows(key, rows, count, picks):
    scores = jax.random.randint(key, (rows, count - 1), 0, 1 << 20) * count + jnp.arange(count - 1, dtype=jnp.int32)[None, :]
    order = jnp.argsort(scores, axis=1)
    return order[:, :picks].astype(jnp.int32)


def draw_leaf_partners(key, part):
    offsets = distinct_rows(jax.random.fold_in(key, 11), LEAVES, N_NARROW, K_LEAF)
    own = jnp.arange(LEAVES, dtype=jnp.int32) % N_NARROW
    return ((own[:, None] + 1 + offsets) % N_NARROW).astype(jnp.int32)


def draw_parent_partners(key, part):
    offsets = distinct_rows(jax.random.fold_in(key, 23), N_WIDE, N_WIDE, K_TOP)
    own = jnp.arange(N_WIDE, dtype=jnp.int32)
    return ((own[:, None] + 1 + offsets) % N_WIDE).astype(jnp.int32)


def draw_vectors(key, part):
    first = jax.random.fold_in(jax.random.fold_in(key, 37), 0)
    rise = 1.0 + 2.0 * jnp.arange(NPTS, dtype=jnp.float32) / NPTS
    base = jnp.clip(jax.random.normal(first, (NPTS, NVEC), jnp.float32), -4.0, 4.0)
    return base * rise[:, None]


def level_of(stream_key, extent, pieces, low, largest):
    loudness = 1.0
    for axis_at, shards_of in pieces:
        draws = jax.random.uniform(jax.random.fold_in(jax.random.fold_in(stream_key, 6), axis_at), (shards_of,), jnp.float32, low / len(pieces), largest / len(pieces))
        loudness = loudness * jnp.repeat(jnp.exp(draws), extent[axis_at] // shards_of).reshape((-1,) + (1,) * (len(extent) - 1 - axis_at))
    return loudness


def noise(own_key, extent, spread, most, cuts=(), kind=jnp.bfloat16):
    result = spread * jax.random.normal(own_key, extent, jnp.float32)
    if cuts:
        result = result * level_of(own_key, extent, cuts, -0.22, 0.18)
    return jnp.clip(result, -most, most).astype(kind)


def setup_inputs(seed: int = 0) -> dict:
    key_list = jax.random.split(jax.random.key(seed), 10)
    vectors = draw_vectors(jax.random.fold_in(key_list[9], 71), 0)
    near_blocks = noise(key_list[1], (NBLK, 3, BLK, BLK), (3 * BLK) ** -0.5, 0.15625, ((0, 256),))
    leaf_basis = noise(key_list[2], (NPTS, R), NPTS_DEV ** -0.5, 0.125, ((0, 256),))
    transfer = noise(key_list[3], (LEAVES, R, R), (R * N_NARROW) ** -0.5, 0.09375, ((0, 256),))
    leaf_coupling = noise(key_list[4], (LEAVES, K_LEAF, R, R), (R * K_LEAF) ** -0.5, 0.15625, ((0, 256),))
    leaf_partners = draw_leaf_partners(jax.random.fold_in(key_list[9], 71), 0)
    parent_coupling = noise(key_list[6], (N_WIDE, K_TOP, R, R), (R * K_TOP) ** -0.5, 0.21875, ((0, 16),))
    parent_partners = draw_parent_partners(jax.random.fold_in(key_list[9], 71), 0)
    shifts = jnp.clip(jax.random.uniform(key_list[8], (NVEC,), jnp.float32, -1.0, 1.0), -1.0, 1.0)
    return dict(vectors=vectors, near_blocks=near_blocks, leaf_basis=leaf_basis, transfer=transfer, leaf_coupling=leaf_coupling, leaf_partners=leaf_partners, parent_coupling=parent_coupling, parent_partners=parent_partners, shifts=shifts)


def leaf_local(args):
    blocks, extended, basis, vin = args
    fields = extended.reshape(BLOCKS_DEV + 2, BLK, NVEC).astype(jnp.float32)
    wide_blocks = blocks.astype(jnp.float32)
    near = jnp.einsum('bij,bjv->biv', wide_blocks[:, 0], fields[:-2])
    near = near + jnp.einsum('bij,bjv->biv', wide_blocks[:, 1], fields[1:-1])
    near = near + jnp.einsum('bij,bjv->biv', wide_blocks[:, 2], fields[2:])
    coeff = jnp.dot(basis.T, vin, preferred_element_type=jnp.float32)
    return (near.reshape(NPTS_DEV, NVEC), coeff)

def sibling_term(args):
    coupling, picked = args
    return jnp.einsum('jrs,jsv->rv', coupling.astype(jnp.float32), picked.astype(jnp.float32))

def upward_term(args):
    matrix, coeff = args
    return jnp.dot(matrix.T, coeff, preferred_element_type=jnp.float32)

def downward_term(args):
    matrix, values = args
    return jnp.dot(matrix, values, preferred_element_type=jnp.float32)

def apply_operator(field, near_blocks, leaf_basis, transfer, leaf_coupling, leaf_partners, parent_coupling, parent_partners):
    vin = field.astype(jnp.bfloat16).reshape(LEAVES, NPTS_DEV, NVEC)
    zeros = jnp.zeros((1, BLK, NVEC), jnp.bfloat16)
    before = jnp.concatenate([zeros, vin[:-1, NPTS_DEV - BLK:]], axis=0)
    after = jnp.concatenate([vin[1:, :BLK], zeros], axis=0)
    extended = jnp.concatenate([before, vin, after], axis=1)
    blocks = near_blocks.reshape(LEAVES, BLOCKS_DEV, 3, BLK, BLK)
    basis = leaf_basis.reshape(LEAVES, NPTS_DEV, R)
    near, coeff = lax.map(leaf_local, (blocks, extended, basis, vin))
    coeff_b = coeff.astype(jnp.bfloat16)
    group = jnp.arange(LEAVES, dtype=jnp.int32) // N_NARROW
    indices = (group[:, None] * N_NARROW + leaf_partners).astype(jnp.int32)
    picked = coeff_b[indices]
    leaf_far = lax.map(sibling_term, (leaf_coupling, picked))
    upward = lax.map(upward_term, (transfer, coeff_b))
    parent_coeff = lax.optimization_barrier(jnp.sum(upward.reshape(N_WIDE, N_NARROW, R, NVEC), axis=1)).astype(jnp.bfloat16)
    top_picked = parent_coeff[parent_partners].astype(jnp.float32)
    parent_out = jnp.einsum('pjrs,pjsv->prv', parent_coupling.astype(jnp.float32), top_picked).astype(jnp.bfloat16)
    downward = lax.map(downward_term, (transfer, parent_out[group]))
    far_coeff = (leaf_far + downward).astype(jnp.bfloat16)
    far = lax.map(downward_term, (basis, far_coeff))
    return (near + far).reshape(NPTS, NVEC)

def reference(vectors, near_blocks, leaf_basis, transfer, leaf_coupling, leaf_partners, parent_coupling, parent_partners, shifts):
    operands = (near_blocks, leaf_basis, transfer, leaf_coupling, leaf_partners, parent_coupling, parent_partners)
    previous = vectors
    current = apply_operator(vectors, *operands) - shifts[None, :] * vectors
    for step in range(1, DEGREE):
        following = 2.0 * (apply_operator(current, *operands) - shifts[None, :] * current) - previous
        previous, current = (current, following)
    meansq = lax.optimization_barrier(jnp.mean(current * current, axis=0))
    return current / jnp.sqrt(meansq + 1e-06)[None, :]
```

```python
import functools

import jax
import jax.numpy as jnp
from jax import lax
from jax.experimental import pallas as pl
from jax.experimental.pallas import tpu as pltpu
from jax.sharding import Mesh
from jax.sharding import PartitionSpec as P

BLK = 512
DEGREE = 3
ALL = ("wide_0", "wide_1", "narrow_0", "narrow_1")
NARROW = ("narrow_0", "narrow_1")
WIDE = ("wide_0", "wide_1")
F32 = jnp.float32
BF16 = jnp.bfloat16
VMEM = pl.BlockSpec(memory_space=pltpu.VMEM)
SMEM = pl.BlockSpec(memory_space=pltpu.SMEM)


def params(mib=16):
    return pltpu.CompilerParams(vmem_limit_bytes=mib * 1024 * 1024)


def cost(flops, moved):
    return pl.CostEstimate(flops=int(flops), bytes_accessed=int(moved), transcendentals=0)


def dot_nn(a, b):
    return lax.dot_general(a, b, (((1,), (0,)), ((), ())), preferred_element_type=F32)


def dot_nt(a, b):
    return lax.dot_general(a, b, (((1,), (1,)), ((), ())), preferred_element_type=F32)


def send_up(v, basis_ref, transfer_ref, coeff_ref, up_ref, low_ref, high_ref):
    rows = v.shape[1]
    low_ref[...] = v[:, :BLK]
    high_ref[...] = v[:, rows - BLK :]
    coeff = dot_nn(v, basis_ref[...]).astype(BF16)
    up = dot_nn(coeff, transfer_ref[...]).astype(BF16)
    up_ref[...] = up.reshape(up_ref.shape)
    for copy in range(coeff_ref.shape[0]):
        coeff_ref[copy] = coeff


def begin_kernel(vec_ref, basis_ref, transfer_ref, t_ref, v_ref, coeff_ref, up_ref, low_ref, high_ref):
    t = vec_ref[...].T
    t_ref[...] = t
    v = t.astype(BF16)
    v_ref[...] = v
    send_up(v, basis_ref, transfer_ref, coeff_ref, up_ref, low_ref, high_ref)


def near_kernel(first, blocks_ref, v_ref, low_ref, high_ref, t_ref, shift_ref, *rest):
    out_ref = rest[-1]
    b, last = pl.program_id(0), pl.num_programs(0) - 1
    here = pl.ds(pl.multiple_of(b * BLK, BLK), BLK)
    below = pl.ds(pl.multiple_of(jnp.maximum(b - 1, 0) * BLK, BLK), BLK)
    above = pl.ds(pl.multiple_of(jnp.minimum(b + 1, last) * BLK, BLK), BLK)
    low = jnp.where(b == 0, low_ref[...], v_ref[:, below])
    high = jnp.where(b == last, high_ref[...], v_ref[:, above])
    near = dot_nt(low, blocks_ref[0, 0])
    near = near + dot_nt(v_ref[:, here], blocks_ref[0, 1])
    near = near + dot_nt(high, blocks_ref[0, 2])
    value = near - shift_ref[...] * t_ref[:, here]
    if not first:
        value = 2.0 * value - rest[0][:, here]
    out_ref[...] = value


def share_kernel(got_ref, out_ref):
    total = jnp.sum(got_ref[...].astype(F32), axis=0).astype(BF16)
    for copy in range(out_ref.shape[0]):
        out_ref[copy] = total


def parent_kernel(partner_ref, got_ref, coupling_ref, out_ref):
    total = dot_nt(got_ref[partner_ref[0]], coupling_ref[0])
    for j in range(1, coupling_ref.shape[0]):
        total = total + dot_nt(got_ref[partner_ref[j]], coupling_ref[j])
    total = total.astype(BF16)
    for copy in range(out_ref.shape[0]):
        out_ref[copy] = total


def sibling_kernel(partner_ref, core_ref, own_ref, other_ref, coupling_ref, out_ref):
    total = None
    for j in range(coupling_ref.shape[0]):
        leaf = partner_ref[j]
        chip = leaf // 2
        picked = jnp.where(leaf % 2 == core_ref[0], own_ref[chip], other_ref[chip])
        term = dot_nt(picked, coupling_ref[j])
        total = term if total is None else total + term
    out_ref[...] = total


def advanced(scale, part_ref, far_ref, parent_ref, transfer_ref, basis_ref):
    parent = parent_ref[...].reshape(far_ref.shape)
    far = (far_ref[...] + dot_nt(parent, transfer_ref[...])).astype(BF16)
    return part_ref[...] + scale * dot_nt(far, basis_ref[...])


def step_kernel(scale, part_ref, far_ref, parent_ref, transfer_ref, basis_ref, t_ref, v_ref, coeff_ref, up_ref, low_ref, high_ref):
    t = advanced(scale, part_ref, far_ref, parent_ref, transfer_ref, basis_ref)
    t_ref[...] = t
    v = t.astype(BF16)
    v_ref[...] = v
    send_up(v, basis_ref, transfer_ref, coeff_ref, up_ref, low_ref, high_ref)


def final_kernel(scale, part_ref, far_ref, parent_ref, transfer_ref, basis_ref, t_ref, squares_ref):
    t = advanced(scale, part_ref, far_ref, parent_ref, transfer_ref, basis_ref)
    t_ref[...] = t
    columns, rows = t.shape
    sums = t[:, :128] * t[:, :128]
    for k in range(1, rows // 128):
        piece = t[:, k * 128 : (k + 1) * 128]
        sums = sums + piece * piece
    row = jnp.sum(sums.T, axis=0, keepdims=True)
    for copy in range(squares_ref.shape[0]):
        squares_ref[copy] = jnp.broadcast_to(row, squares_ref.shape[1:])


def turn_kernel(t_ref, out_ref):
    out_ref[...] = t_ref[...].T


def gather_kernel(got_ref, out_ref):
    total = jnp.sum(got_ref[...], axis=0)
    for copy in range(out_ref.shape[0]):
        out_ref[copy] = total


def scale_kernel(total_rows, t_ref, got_ref, out_ref):
    squares = jnp.sum(got_ref[...], axis=0)[:1]
    out_ref[...] = t_ref[...] / jnp.sqrt(squares / total_rows + 1e-06)


def call(kernel, outs, operands, specs=None, flops=1e6, moved=1e6, mib=16, name=None):
    return pl.pallas_call(
        kernel,
        out_shape=[jax.ShapeDtypeStruct(s, d) for s, d in outs],
        in_specs=specs or [VMEM] * len(operands),
        out_specs=[VMEM] * len(outs),
        compiler_params=params(mib),
        cost_estimate=cost(flops, moved),
        name=name,
    )(*operands)


def exchanged(pieces, axes):
    return lax.all_to_all(pieces, axes, split_axis=0, concat_axis=0, tiled=True)


def shards(vectors, near_blocks, leaf_basis, transfer, leaf_coupling, leaf_partners, parent_coupling, parent_partners, shifts):
    rows, cols = vectors.shape
    rank = leaf_basis.shape[1]
    blocks = near_blocks.shape[0]
    n_narrow, n_wide = lax.axis_size(NARROW), lax.axis_size(WIDE)
    n_chips = lax.axis_size("narrow_0")
    devices = n_narrow * n_wide
    part = cols // n_narrow
    matrix = transfer[0]
    core = lax.axis_index("narrow_1").astype(jnp.int32)[None]
    shift = shifts[:, None]
    up = [(i, i + 1) for i in range(devices - 1)]
    down = [(b, a) for a, b in up]
    state = [
        ((cols, rows), F32),
        ((cols, rows), BF16),
        ((n_chips, cols, rank), BF16),
        ((n_narrow, part, rank), BF16),
        ((cols, BLK), BF16),
        ((cols, BLK), BF16),
    ]
    leaf_flops = 2 * 2 * rows * rank * cols

    def near_part(previous, t, v, low, high):
        whole = lambda shape: pl.BlockSpec(shape, lambda b: (0,) * len(shape))
        operands = [near_blocks, v, low, high, t, shift] + ([] if previous is None else [previous])
        return pl.pallas_call(
            functools.partial(near_kernel, previous is None),
            grid=(blocks,),
            out_shape=jax.ShapeDtypeStruct((cols, rows), F32),
            in_specs=[pl.BlockSpec((1, 3, BLK, BLK), lambda b: (b, 0, 0, 0))] + [whole(o.shape) for o in operands[1:]],
            out_specs=pl.BlockSpec((cols, BLK), lambda b: (0, b)),
            compiler_params=params(),
            cost_estimate=cost(2 * 3 * blocks * BLK * BLK * cols, 2 * near_blocks.size),
            name="near",
        )(*operands)

    previous = None
    t, v, coeff, upward, low, high = call(begin_kernel, state, (vectors, leaf_basis, matrix), flops=leaf_flops, name="begin")
    for step in range(DEGREE):
        scale = 1.0 if step == 0 else 2.0
        arrived = exchanged(upward, NARROW)
        own = exchanged(coeff, "narrow_0")
        low_in = lax.ppermute(high, ALL, up)
        high_in = lax.ppermute(low, ALL, down)
        (share,) = call(share_kernel, [((n_wide, part, rank), BF16)], (arrived,), name="share")
        gathered = exchanged(share, WIDE)
        value = near_part(previous, t, v, low_in, high_in)
        other = lax.ppermute(own, "narrow_1", [(0, 1), (1, 0)])
        (parent,) = call(
            parent_kernel,
            [((n_narrow, part, rank), BF16)],
            (parent_partners[0], gathered, parent_coupling[0]),
            [SMEM, VMEM, VMEM],
            name="parent",
        )
        parent_out = exchanged(parent, NARROW)
        (far,) = call(
            sibling_kernel,
            [((cols, rank), F32)],
            (leaf_partners[0], core, own, other, leaf_coupling[0]),
            [SMEM, SMEM, VMEM, VMEM, VMEM],
            flops=6 * 2 * rank * rank * cols,
            name="sibling",
        )
        operands = (value, far, parent_out, matrix, leaf_basis)
        previous = t
        if step < DEGREE - 1:
            t, v, coeff, upward, low, high = call(
                functools.partial(step_kernel, scale), state, operands, flops=2 * leaf_flops, name="advance"
            )
        else:
            t, squares = call(
                functools.partial(final_kernel, scale),
                [((cols, rows), F32), ((n_narrow, 8, cols), F32)],
                operands,
                flops=leaf_flops,
                name="final",
            )
    (turned,) = call(turn_kernel, [((rows, cols), F32)], (t,), flops=4e8, name="turn")
    sums = exchanged(squares, NARROW)
    (sums,) = call(gather_kernel, [((n_wide, 8, cols), F32)], (sums,), name="gather")
    sums = exchanged(sums, WIDE)
    (out,) = call(functools.partial(scale_kernel, rows * devices), [((rows, cols), F32)], (turned, sums), name="scale")
    return out


def solution(mesh):
    finer = Mesh(mesh.devices.reshape(4, 4, 8, 2), ALL)
    placed = (
        P(ALL, None),
        P(ALL, None, None, None),
        P(ALL, None),
        P(ALL, None, None),
        P(ALL, None, None, None),
        P(ALL, None),
        P(WIDE, None, None, None),
        P(WIDE, None),
        P(),
    )
    return jax.shard_map(shards, mesh=finer, in_specs=placed, out_specs=P(ALL, None), check_vma=False)
```

```python
import functools

import jax
import jax.numpy as jnp
from jax import lax
from jax.experimental import pallas as pl
from jax.experimental.pallas import tpu as pltpu
from jax.sharding import Mesh
from jax.sharding import PartitionSpec as P


BLK = 512
DEGREE = 3
ALL = ("wide_0", "wide_1", "narrow_0", "narrow_1")
NARROW = ("narrow_0", "narrow_1")
WIDE = ("wide_0", "wide_1")
F32 = jnp.float32
BF16 = jnp.bfloat16
VMEM = pl.BlockSpec(memory_space=pltpu.VMEM)
SMEM = pl.BlockSpec(memory_space=pltpu.SMEM)


def cost(flops, moved):
    return pl.CostEstimate(flops=int(flops), bytes_accessed=int(moved), transcendentals=0)


def dot_nn(a, b):
    return lax.dot_general(a, b, (((1,), (0,)), ((), ())), preferred_element_type=F32)


def dot_nt(a, b):
    return lax.dot_general(a, b, (((1,), (1,)), ((), ())), preferred_element_type=F32)


def send_up(t, basis_ref, transfer_ref, v_ref, coeff_ref, up_ref, low_ref, high_ref, sum_ref):
    b, last = pl.program_id(0), pl.num_programs(0) - 1
    v = t.astype(BF16)
    v_ref[...] = v
    part = dot_nn(t.T.astype(BF16), basis_ref[...])

    @pl.when(b == 0)
    def _():
        sum_ref[...] = part
        low_ref[...] = v

    @pl.when(b > 0)
    def _():
        sum_ref[...] += part

    @pl.when(b == last)
    def _():
        high_ref[...] = v
        coeff = sum_ref[...].astype(BF16)
        coeff_ref[...] = coeff
        up_ref[...] = dot_nn(coeff, transfer_ref[...]).astype(BF16).reshape(up_ref.shape)


def begin_kernel(vec_ref, basis_ref, transfer_ref, *rest):
    send_up(vec_ref[...], basis_ref, transfer_ref, *rest)


def near_kernel(first, blocks_ref, v_ref, low_ref, high_ref, t_ref, shift_ref, *rest):
    out_ref = rest[-1]
    b, last = pl.program_id(0), pl.num_programs(0) - 1
    here = pl.ds(pl.multiple_of(b * BLK, BLK), BLK)
    below = pl.ds(pl.multiple_of(jnp.maximum(b - 1, 0) * BLK, BLK), BLK)
    above = pl.ds(pl.multiple_of(jnp.minimum(b + 1, last) * BLK, BLK), BLK)
    low = jnp.where(b == 0, low_ref[...], v_ref[below, :])
    high = jnp.where(b == last, high_ref[...], v_ref[above, :])
    near = dot_nn(blocks_ref[0, 0], low)
    near = near + dot_nn(blocks_ref[0, 1], v_ref[here, :])
    near = near + dot_nn(blocks_ref[0, 2], high)
    value = near - shift_ref[...] * t_ref[...]
    if not first:
        value = 2.0 * value - rest[0][...]
    out_ref[...] = value


def share_kernel(got_ref, out_ref):
    total = jnp.sum(got_ref[...].astype(F32), axis=0).astype(BF16)
    for copy in range(out_ref.shape[0]):
        out_ref[copy] = total


def parent_kernel(partner_ref, got_ref, coupling_ref, out_ref):
    total = dot_nt(got_ref[partner_ref[0]], coupling_ref[0])
    for j in range(1, coupling_ref.shape[0]):
        total = total + dot_nt(got_ref[partner_ref[j]], coupling_ref[j])
    total = total.astype(BF16)
    for copy in range(out_ref.shape[0]):
        out_ref[copy] = total


def pack_kernel(*refs):
    at = 0
    for ref in refs[:-1]:
        refs[-1][at : at + ref.shape[0]] = ref[...]
        at += ref.shape[0]


def pair_kernel(own_ref, other_ref, out_ref):
    out_ref[0] = own_ref[...]
    out_ref[1] = other_ref[...]


def sibling_kernel(partner_ref, pair_ref, mine_ref, theirs_ref, coupling_ref, out_ref):
    chips = lax.axis_size("narrow_0")
    chip, core = lax.axis_index("narrow_0"), lax.axis_index("narrow_1")
    half = chips // 2
    end = chips - 2
    total = None
    for j in range(coupling_ref.shape[0]):
        leaf = partner_ref[j]
        parity = lax.rem(leaf, 2)
        away = lax.rem(chip - leaf // 2 + chips, chips)
        low_side = jnp.logical_or(away < half, jnp.logical_and(away == half, parity == 0))
        low_at = jnp.where(away == half, end, 2 * (away - 1) + parity)
        high_at = jnp.where(away == half, end, 2 * (chips - 1 - away) + 1 - parity)
        at = jnp.where(low_side, low_at, high_at)
        at = jnp.minimum(jnp.maximum(at, 0), end)
        is_mine = low_side == (core == 0)
        from_ring = jnp.where(is_mine, mine_ref[at], theirs_ref[at])
        from_pair = pair_ref[jnp.where(parity == core, 0, 1)]
        term = dot_nt(jnp.where(away == 0, from_pair, from_ring), coupling_ref[j])
        total = term if total is None else total + term
    out_ref[...] = total


def advanced(scale, part_ref, far_ref, parent_ref, transfer_ref, basis_ref, far_out):
    @pl.when(pl.program_id(0) == 0)
    def _():
        parent = parent_ref[...].reshape(far_ref.shape)
        far = far_ref[...] + dot_nt(parent, transfer_ref[...])
        far_out[...] = far.T.astype(BF16)

    return part_ref[...] + scale * dot_nn(basis_ref[...], far_out[...])


def step_kernel(scale, part_ref, far_ref, parent_ref, transfer_ref, basis_ref, t_ref, *rest):
    t = advanced(scale, part_ref, far_ref, parent_ref, transfer_ref, basis_ref, rest[-1])
    t_ref[...] = t
    send_up(t, basis_ref, transfer_ref, *rest[:-1])


def final_kernel(scale, part_ref, far_ref, parent_ref, transfer_ref, basis_ref, out_ref, squares_ref, far_out, sum_ref):
    b, last = pl.program_id(0), pl.num_programs(0) - 1
    t = advanced(scale, part_ref, far_ref, parent_ref, transfer_ref, basis_ref, far_out)
    out_ref[...] = t
    part = jnp.sum((t * t).reshape(t.shape[0] // 8, 8, t.shape[1]), axis=0)

    @pl.when(b == 0)
    def _():
        sum_ref[...] = part

    @pl.when(b > 0)
    def _():
        sum_ref[...] += part

    @pl.when(b == last)
    def _():
        for copy in range(squares_ref.shape[0]):
            squares_ref[copy] = sum_ref[...]


def gather_kernel(got_ref, out_ref):
    total = jnp.sum(got_ref[...], axis=0)
    for copy in range(out_ref.shape[0]):
        out_ref[copy] = total


def scale_kernel(total_rows, t_ref, got_ref, out_ref):
    squares = jnp.sum(jnp.sum(got_ref[...], axis=0), axis=0, keepdims=True)
    out_ref[...] = t_ref[...] / jnp.sqrt(squares / total_rows + 1e-06)


def whole(shape):
    return pl.BlockSpec(shape, lambda b: (0,) * len(shape))


def by_rows(shape):
    return pl.BlockSpec((BLK, shape[1]), lambda b: (b, 0))


def call(kernel, outs, operands, specs=None, flops=1e6, moved=1e6):
    return pl.pallas_call(
        kernel,
        out_shape=[jax.ShapeDtypeStruct(s, d) for s, d in outs],
        in_specs=specs or [VMEM] * len(operands),
        out_specs=[VMEM] * len(outs),
        compiler_params=pltpu.CompilerParams(vmem_limit_bytes=8 * 1024 * 1024),
        cost_estimate=cost(flops, moved),
    )(*operands)


def stream(kernel, grid, outs, operands, flops, scratch):
    return pl.pallas_call(
        kernel,
        grid=(grid,),
        out_shape=[jax.ShapeDtypeStruct(s, d) for s, d, _ in outs],
        in_specs=[cut(o.shape) for o, cut in operands],
        out_specs=[cut(s) for s, _, cut in outs],
        scratch_shapes=scratch,
        cost_estimate=cost(flops, sum(o.size * o.dtype.itemsize for o, _ in operands)),
    )(*[o for o, _ in operands])


def exchanged(pieces, axes):
    return lax.all_to_all(pieces, axes, split_axis=0, concat_axis=0, tiled=True)


def shards(vectors, near_blocks, leaf_basis, transfer, leaf_coupling, leaf_partners, parent_coupling, parent_partners, shifts):
    rows, cols = vectors.shape
    rank = leaf_basis.shape[1]
    blocks = near_blocks.shape[0]
    n_narrow, n_wide = lax.axis_size(NARROW), lax.axis_size(WIDE)
    chips = lax.axis_size("narrow_0")
    devices = n_narrow * n_wide
    part = cols // n_narrow
    matrix = transfer[0]
    shift = shifts[None, :]
    up = [(i, i + 1) for i in range(devices - 1)]
    down = [(b, a) for a, b in up]
    swap = [(0, 1), (1, 0)]
    state = [
        ((rows, cols), BF16, by_rows),
        ((cols, rank), BF16, whole),
        ((n_narrow, part, rank), BF16, whole),
        ((BLK, cols), BF16, whole),
        ((BLK, cols), BF16, whole),
    ]
    sums = pltpu.VMEM((cols, rank), F32)
    fars = pltpu.VMEM((rank, cols), BF16)
    leaf_flops = 2 * 2 * rows * rank * cols

    def away(s):
        there = [((2 * c), 2 * ((c + s) % chips)) for c in range(chips)]
        back = [((2 * c + 1), 2 * ((c - s) % chips) + 1) for c in range(chips)]
        return there + back

    previous, t = None, vectors
    v, coeff, upward, low, high = stream(
        begin_kernel, blocks, state, ((vectors, by_rows), (leaf_basis, by_rows), (matrix, whole)), leaf_flops, [sums]
    )
    for step in range(DEGREE):
        scale = 1.0 if step == 0 else 2.0
        arrived = exchanged(upward, NARROW)
        partner = lax.ppermute(coeff, "narrow_1", swap)
        low_in = lax.ppermute(high, ALL, up)
        high_in = lax.ppermute(low, ALL, down)
        operands = [(near_blocks, lambda shape: pl.BlockSpec((1, *shape[1:]), lambda b: (b, 0, 0, 0)))]
        operands += [(v, whole), (low_in, whole), (high_in, whole), (t, by_rows), (shift, whole)]
        operands += [] if previous is None else [(previous, by_rows)]
        (value,) = stream(
            functools.partial(near_kernel, previous is None),
            blocks,
            [((rows, cols), F32, by_rows)],
            operands,
            2 * 3 * blocks * BLK * BLK * cols,
            [],
        )
        (share,) = call(share_kernel, [((n_wide, part, rank), BF16)], (arrived,))
        gathered = exchanged(share, WIDE)
        (pair,) = call(pair_kernel, [((2, cols, rank), BF16)], (coeff, partner))
        ring = []
        for s in range(1, chips // 2 + 1):
            ring.append(lax.ppermute(pair if s < chips // 2 else coeff[None], NARROW, away(s)))
        (parent,) = call(
            parent_kernel,
            [((n_narrow, part, rank), BF16)],
            (parent_partners[0], gathered, parent_coupling[0]),
            [SMEM, VMEM, VMEM],
        )
        parent_out = exchanged(parent, NARROW)
        (mine,) = call(pack_kernel, [((2 * (chips // 2) - 1, cols, rank), BF16)], ring)
        theirs = lax.ppermute(mine, "narrow_1", swap)
        (far,) = call(
            sibling_kernel,
            [((cols, rank), F32)],
            (leaf_partners[0], pair, mine, theirs, leaf_coupling[0]),
            [SMEM, VMEM, VMEM, VMEM, VMEM],
            flops=6 * 2 * rank * rank * cols,
        )
        operands = ((value, by_rows), (far, whole), (parent_out, whole), (matrix, whole), (leaf_basis, by_rows))
        previous = t
        if step < DEGREE - 1:
            t, v, coeff, upward, low, high = stream(
                functools.partial(step_kernel, scale), blocks, [((rows, cols), F32, by_rows)] + state, operands, 2 * leaf_flops, [sums, fars]
            )
        else:
            out, squares = stream(
                functools.partial(final_kernel, scale),
                blocks,
                [((rows, cols), F32, by_rows), ((n_narrow, 8, cols), F32, whole)],
                operands,
                leaf_flops,
                [fars, pltpu.VMEM((8, cols), F32)],
            )
    squares = exchanged(squares, NARROW)
    (squares,) = call(gather_kernel, [((n_wide, 8, cols), F32)], (squares,))
    squares = exchanged(squares, WIDE)
    (out,) = stream(
        functools.partial(scale_kernel, rows * devices),
        blocks,
        [((rows, cols), F32, by_rows)],
        ((out, by_rows), (squares, whole)),
        1e6,
        [],
    )
    return out


def solution(mesh):
    finer = Mesh(mesh.devices.reshape(4, 4, 8, 2), ALL)
    placed = (
        P(ALL, None),
        P(ALL, None, None, None),
        P(ALL, None),
        P(ALL, None, None),
        P(ALL, None, None, None),
        P(ALL, None),
        P(WIDE, None, None, None),
        P(WIDE, None),
        P(),
    )
    return jax.shard_map(shards, mesh=finer, in_specs=placed, out_specs=P(ALL, None), check_vma=False)
```

```python
import functools

import jax
import jax.numpy as jnp
from jax import lax
from jax.experimental import pallas as pl
from jax.experimental.pallas import tpu as pltpu
from jax.sharding import Mesh
from jax.sharding import PartitionSpec as P


BLK = 512
DEGREE = 3
ALL = ("wide_0", "wide_1", "narrow_0", "narrow_1")
NARROW = ("narrow_0", "narrow_1")
WIDE = ("wide_0", "wide_1")
F32 = jnp.float32
BF16 = jnp.bfloat16
VMEM = pl.BlockSpec(memory_space=pltpu.VMEM)
SMEM = pl.BlockSpec(memory_space=pltpu.SMEM)


def cost(flops, moved):
    return pl.CostEstimate(flops=int(flops), bytes_accessed=int(moved), transcendentals=0)


def dot_nn(a, b):
    return lax.dot_general(a, b, (((1,), (0,)), ((), ())), preferred_element_type=F32)


def dot_nt(a, b):
    return lax.dot_general(a, b, (((1,), (1,)), ((), ())), preferred_element_type=F32)


def block(b):
    return slice(b * BLK, (b + 1) * BLK)


def begin_kernel(vec_ref, basis_ref, transfer_ref, v_ref, load_ref, low_ref, high_ref):
    blocks, rank = vec_ref.shape[0] // BLK, basis_ref.shape[1]
    total = None
    for b in range(blocks):
        t = vec_ref[block(b), :]
        v = t.astype(BF16)
        v_ref[block(b), :] = v
        if b == 0:
            low_ref[...] = v
        if b == blocks - 1:
            high_ref[...] = v
        term = dot_nn(t.T.astype(BF16), basis_ref[block(b), :])
        total = term if total is None else total + term
    load_ref[:rank] = transfer_ref[...]
    load_ref[rank:] = total.astype(BF16)


def near_kernel(first, blocks_ref, v_ref, low_ref, high_ref, t_ref, shift_ref, *rest):
    out_ref = rest[-1]
    blocks = blocks_ref.shape[0]
    for b in range(blocks):
        near = dot_nn(blocks_ref[b, 0], low_ref[...] if b == 0 else v_ref[block(b - 1), :])
        near = near + dot_nn(blocks_ref[b, 1], v_ref[block(b), :])
        near = near + dot_nn(blocks_ref[b, 2], high_ref[...] if b == blocks - 1 else v_ref[block(b + 1), :])
        value = near - shift_ref[...] * t_ref[block(b), :]
        if not first:
            value = 2.0 * value - rest[0][block(b), :]
        out_ref[block(b), :] = value


def share_kernel(base, count, *refs):
    matrices, loads, out_ref = refs[:count], refs[count:-1], refs[-1]
    half, rank = out_ref.shape[1:]
    start = pl.multiple_of(base + lax.axis_index("narrow_1") * half, half)
    total = None
    for matrix_ref, load_ref in zip(matrices, loads):
        for slot in range(2):
            term = dot_nn(load_ref[slot, pl.ds(start, half), :], matrix_ref[slot, :rank, :])
            total = term if total is None else total + term
    total = total.astype(BF16)
    for copy in range(out_ref.shape[0]):
        out_ref[copy] = total


def parent_kernel(partner_ref, got_ref, coupling_ref, out_ref):
    total = dot_nt(got_ref[partner_ref[0]], coupling_ref[0])
    for j in range(1, coupling_ref.shape[0]):
        total = total + dot_nt(got_ref[partner_ref[j]], coupling_ref[j])
    out_ref[...] = total.astype(BF16)


def pair_kernel(own_ref, other_ref, out_ref):
    out_ref[0] = own_ref[...]
    out_ref[1] = other_ref[...]


def sibling_kernel(base, count, partner_ref, *refs):
    loads, (coupling_ref, out_ref, held) = refs[:count], refs[count:]
    for k, load_ref in enumerate(loads):
        for slot in range(2):
            held[2 * k + slot] = load_ref[slot, base:, :]
    chips = lax.axis_size("narrow_0")
    chip, core = lax.axis_index("narrow_0"), lax.axis_index("narrow_1")
    half = chips // 2
    total = None
    for j in range(coupling_ref.shape[0]):
        leaf = partner_ref[j]
        parity = lax.rem(leaf, 2)
        away = lax.rem(chip - leaf // 2 + chips, chips)
        own_ring = jnp.logical_or(away == 0, away == half)
        ring_core = jnp.where(own_ring, core, jnp.where(away < half, 0, 1))
        hops = jnp.where(away <= half, away, chips - away)
        at = jnp.where(ring_core == core, hops, half + hops)
        at = 2 * at + jnp.where(parity == ring_core, 0, 1)
        term = dot_nt(held[at], coupling_ref[j])
        total = term if total is None else total + term
    out_ref[...] = total


def far_of(far_ref, mine_ref, theirs_ref, transfer_ref):
    mine, theirs = dot_nt(mine_ref[...], transfer_ref[...]), dot_nt(theirs_ref[...], transfer_ref[...])
    first = lax.axis_index("narrow_1") == 0
    down = jnp.concatenate([jnp.where(first, mine, theirs), jnp.where(first, theirs, mine)], axis=0)
    return (far_ref[...] + down).T.astype(BF16)


def step_kernel(
    scale, part_ref, far_ref, mine_ref, theirs_ref, transfer_ref, basis_ref, t_ref, v_ref, load_ref, low_ref, high_ref
):
    blocks = part_ref.shape[0] // BLK
    far = far_of(far_ref, mine_ref, theirs_ref, transfer_ref)
    total = None
    for b in range(blocks):
        basis = basis_ref[block(b), :]
        t = part_ref[block(b), :] + scale * dot_nn(basis, far)
        t_ref[block(b), :] = t
        v = t.astype(BF16)
        v_ref[block(b), :] = v
        if b == 0:
            low_ref[...] = v
        if b == blocks - 1:
            high_ref[...] = v
        term = dot_nn(t.T.astype(BF16), basis)
        total = term if total is None else total + term
    load_ref[...] = total.astype(BF16)


def final_kernel(scale, part_ref, far_ref, mine_ref, theirs_ref, transfer_ref, basis_ref, out_ref, squares_ref):
    far = far_of(far_ref, mine_ref, theirs_ref, transfer_ref)
    total = None
    for b in range(part_ref.shape[0] // BLK):
        t = part_ref[block(b), :] + scale * dot_nn(basis_ref[block(b), :], far)
        out_ref[block(b), :] = t
        term = jnp.sum((t * t).reshape(BLK // 8, 8, t.shape[1]), axis=0)
        total = term if total is None else total + term
    for copy in range(squares_ref.shape[0]):
        squares_ref[copy] = total


def gather_kernel(got_ref, out_ref):
    total = jnp.sum(got_ref[...], axis=0)
    for copy in range(out_ref.shape[0]):
        out_ref[copy] = total


def scale_kernel(total_rows, t_ref, got_ref, out_ref):
    squares = jnp.sum(jnp.sum(got_ref[...], axis=0), axis=0, keepdims=True)
    out_ref[...] = t_ref[...] / jnp.sqrt(squares / total_rows + 1e-06)


def call(kernel, outs, operands, specs=None, flops=1e6, moved=1e6, scratch=()):
    return pl.pallas_call(
        kernel,
        out_shape=[jax.ShapeDtypeStruct(s, d) for s, d in outs],
        in_specs=specs or [VMEM] * len(operands),
        out_specs=[VMEM] * len(outs),
        scratch_shapes=scratch,
        compiler_params=pltpu.CompilerParams(vmem_limit_bytes=16 * 1024 * 1024),
        cost_estimate=cost(flops, moved),
    )(*operands)


def exchanged(pieces, axes):
    return lax.all_to_all(pieces, axes, split_axis=0, concat_axis=0, tiled=True)


def shards(vectors, near_blocks, leaf_basis, transfer, leaf_coupling, leaf_partners, parent_coupling, parent_partners, shifts):
    rows, cols = vectors.shape
    rank = leaf_basis.shape[1]
    blocks = near_blocks.shape[0]
    n_narrow, n_wide = lax.axis_size(NARROW), lax.axis_size(WIDE)
    chips = lax.axis_size("narrow_0")
    devices = n_narrow * n_wide
    half = cols // 2
    matrix = transfer[0]
    shift = shifts[None, :]
    up = [(i, i + 1) for i in range(devices - 1)]
    down = [(b, a) for a, b in up]
    swap = [(0, 1), (1, 0)]
    count = chips

    def state(size):
        return [((rows, cols), BF16), ((size, rank), BF16), ((BLK, cols), BF16), ((BLK, cols), BF16)]

    leaf_flops = 2 * 2 * rows * rank * cols

    away = [(2 * c, 2 * ((c + 1) % chips)) for c in range(chips)]
    away += [(2 * c + 1, 2 * ((c - 1) % chips) + 1) for c in range(chips)]

    previous, t = None, vectors
    v, load, low, high = call(begin_kernel, state(rank + cols), (vectors, leaf_basis, matrix), flops=leaf_flops)
    matrices = None
    for step in range(DEGREE):
        scale = 1.0 if step == 0 else 2.0
        base = rank if step == 0 else 0
        partner = lax.ppermute(load, "narrow_1", swap)
        (pair,) = call(pair_kernel, [((2, *load.shape), BF16)], (load, partner))
        ring, crossed = [pair], []
        for s in range(1, chips // 2 + 1):
            ring.append(lax.ppermute(ring[-1], NARROW, away))
            if s < chips // 2:
                crossed.append(lax.ppermute(ring[-1], "narrow_1", swap))
        loads = ring + crossed
        matrices = loads if matrices is None else matrices
        low_in = lax.ppermute(high, ALL, up)
        high_in = lax.ppermute(low, ALL, down)
        operands = [near_blocks, v, low_in, high_in, t, shift] + ([] if previous is None else [previous])
        (value,) = call(
            functools.partial(near_kernel, previous is None),
            [((rows, cols), F32)],
            operands,
            flops=2 * 3 * blocks * BLK * BLK * cols,
        )
        (share,) = call(
            functools.partial(share_kernel, base, count),
            [((n_wide, half, rank), BF16)],
            matrices + loads,
            flops=2 * n_narrow * half * rank * rank,
        )
        (far,) = call(
            functools.partial(sibling_kernel, base, count),
            [((cols, rank), F32)],
            (leaf_partners[0], *loads, leaf_coupling[0]),
            [SMEM] + [VMEM] * (count + 1),
            flops=6 * 2 * rank * rank * cols,
            scratch=[pltpu.VMEM((2 * count, cols, rank), BF16)],
        )
        gathered = exchanged(share, WIDE)
        (mine,) = call(
            parent_kernel,
            [((half, rank), BF16)],
            (parent_partners[0], gathered, parent_coupling[0]),
            [SMEM, VMEM, VMEM],
        )
        theirs = lax.ppermute(mine, "narrow_1", swap)
        operands = (value, far, mine, theirs, matrix, leaf_basis)
        previous = t
        if step < DEGREE - 1:
            t, v, load, low, high = call(
                functools.partial(step_kernel, scale),
                [((rows, cols), F32)] + state(cols),
                operands,
                flops=2 * leaf_flops,
            )
        else:
            out, squares = call(
                functools.partial(final_kernel, scale),
                [((rows, cols), F32), ((n_narrow, 8, cols), F32)],
                operands,
                flops=leaf_flops,
            )
    squares = exchanged(squares, NARROW)
    (squares,) = call(gather_kernel, [((n_wide, 8, cols), F32)], (squares,))
    squares = exchanged(squares, WIDE)
    (out,) = call(functools.partial(scale_kernel, rows * devices), [((rows, cols), F32)], (out, squares))
    return out


def solution(mesh):
    finer = Mesh(mesh.devices.reshape(4, 4, 8, 2), ALL)
    placed = (
        P(ALL, None),
        P(ALL, None, None, None),
        P(ALL, None),
        P(ALL, None, None),
        P(ALL, None, None, None),
        P(ALL, None),
        P(WIDE, None, None, None),
        P(WIDE, None),
        P(),
    )
    return jax.shard_map(shards, mesh=finer, in_specs=placed, out_specs=P(ALL, None), check_vma=False)
```

```python
import functools

import jax
import jax.numpy as jnp
from jax import lax
from jax.experimental import pallas as pl
from jax.experimental.pallas import tpu as pltpu
from jax.sharding import Mesh
from jax.sharding import PartitionSpec as P


BLK = 512
DEGREE = 3
ALL = ("wide_0", "wide_1", "narrow_0", "narrow_1")
NARROW = ("narrow_0", "narrow_1")
WIDE = ("wide_0", "wide_1")
F32 = jnp.float32
BF16 = jnp.bfloat16
VMEM = pl.BlockSpec(memory_space=pltpu.VMEM)
SMEM = pl.BlockSpec(memory_space=pltpu.SMEM)


def cost(flops, moved):
    return pl.CostEstimate(flops=int(flops), bytes_accessed=int(moved), transcendentals=0)


def dot_nn(a, b):
    return lax.dot_general(a, b, (((1,), (0,)), ((), ())), preferred_element_type=F32)


def dot_nt(a, b):
    return lax.dot_general(a, b, (((1,), (1,)), ((), ())), preferred_element_type=F32)


def block(b):
    return slice(b * BLK, (b + 1) * BLK)


def send(total, transfer_ref, load_ref):
    coeff = total.astype(BF16)
    load_ref[0] = coeff
    load_ref[1] = dot_nn(coeff, transfer_ref[...]).astype(BF16)


def begin_kernel(vec_ref, basis_ref, transfer_ref, v_ref, load_ref, low_ref, high_ref):
    blocks = vec_ref.shape[0] // BLK
    total = None
    for b in range(blocks):
        t = vec_ref[block(b), :]
        v = t.astype(BF16)
        v_ref[block(b), :] = v
        if b == 0:
            low_ref[...] = v
        if b == blocks - 1:
            high_ref[...] = v
        term = dot_nn(t.T.astype(BF16), basis_ref[block(b), :])
        total = term if total is None else total + term
    send(total, transfer_ref, load_ref)


def near_kernel(first, blocks_ref, v_ref, low_ref, high_ref, t_ref, shift_ref, *rest):
    out_ref = rest[-1]
    blocks = blocks_ref.shape[0]
    for b in range(blocks):
        near = dot_nn(blocks_ref[b, 0], low_ref[...] if b == 0 else v_ref[block(b - 1), :])
        near = near + dot_nn(blocks_ref[b, 1], v_ref[block(b), :])
        near = near + dot_nn(blocks_ref[b, 2], high_ref[...] if b == blocks - 1 else v_ref[block(b + 1), :])
        value = near - shift_ref[...] * t_ref[block(b), :]
        if not first:
            value = 2.0 * value - rest[0][block(b), :]
        out_ref[block(b), :] = value


def share_kernel(*refs):
    loads, out_ref = refs[:-1], refs[-1]
    half = out_ref.shape[1]
    rows = pl.ds(pl.multiple_of(lax.axis_index("narrow_1") * half, half), half)
    total = loads[0][2, rows, :].astype(F32)
    for load_ref in loads[1:]:
        total = total + load_ref[2, rows, :].astype(F32)
    total = total.astype(BF16)
    for copy in range(out_ref.shape[0]):
        out_ref[copy] = total


def parent_kernel(partner_ref, got_ref, coupling_ref, out_ref):
    total = dot_nt(got_ref[partner_ref[0]], coupling_ref[0])
    for j in range(1, coupling_ref.shape[0]):
        total = total + dot_nt(got_ref[partner_ref[j]], coupling_ref[j])
    out_ref[...] = total.astype(BF16)


def pair_kernel(own_ref, other_ref, out_ref):
    out_ref[0] = own_ref[0]
    out_ref[1] = other_ref[0]
    out_ref[2] = (own_ref[1].astype(F32) + other_ref[1].astype(F32)).astype(BF16)


def sibling_kernel(count, partner_ref, *refs):
    loads, (coupling_ref, out_ref, held) = refs[:count], refs[count:]
    for k, load_ref in enumerate(loads):
        for slot in range(2):
            held[2 * k + slot] = load_ref[slot]
    chips = lax.axis_size("narrow_0")
    chip, core = lax.axis_index("narrow_0"), lax.axis_index("narrow_1")
    half = chips // 2
    total = None
    for j in range(coupling_ref.shape[0]):
        leaf = partner_ref[j]
        parity = lax.rem(leaf, 2)
        away = lax.rem(chip - leaf // 2 + chips, chips)
        own_ring = jnp.logical_or(away == 0, away == half)
        ring_core = jnp.where(own_ring, core, jnp.where(away < half, 0, 1))
        hops = jnp.where(away <= half, away, chips - away)
        at = jnp.where(ring_core == core, hops, half + hops)
        at = 2 * at + jnp.where(parity == ring_core, 0, 1)
        term = dot_nt(held[at], coupling_ref[j])
        total = term if total is None else total + term
    out_ref[...] = total


def far_of(far_ref, mine_ref, theirs_ref, transfer_ref):
    mine, theirs = dot_nt(mine_ref[...], transfer_ref[...]), dot_nt(theirs_ref[...], transfer_ref[...])
    first = lax.axis_index("narrow_1") == 0
    down = jnp.concatenate([jnp.where(first, mine, theirs), jnp.where(first, theirs, mine)], axis=0)
    return (far_ref[...] + down).T.astype(BF16)


def step_kernel(
    scale, part_ref, far_ref, mine_ref, theirs_ref, transfer_ref, basis_ref, t_ref, v_ref, load_ref, low_ref, high_ref
):
    blocks = part_ref.shape[0] // BLK
    far = far_of(far_ref, mine_ref, theirs_ref, transfer_ref)
    total = None
    for b in range(blocks):
        basis = basis_ref[block(b), :]
        t = part_ref[block(b), :] + scale * dot_nn(basis, far)
        t_ref[block(b), :] = t
        v = t.astype(BF16)
        v_ref[block(b), :] = v
        if b == 0:
            low_ref[...] = v
        if b == blocks - 1:
            high_ref[...] = v
        term = dot_nn(t.T.astype(BF16), basis)
        total = term if total is None else total + term
    send(total, transfer_ref, load_ref)


def final_kernel(scale, part_ref, far_ref, mine_ref, theirs_ref, transfer_ref, basis_ref, out_ref, squares_ref):
    far = far_of(far_ref, mine_ref, theirs_ref, transfer_ref)
    total = None
    for b in range(part_ref.shape[0] // BLK):
        t = part_ref[block(b), :] + scale * dot_nn(basis_ref[block(b), :], far)
        out_ref[block(b), :] = t
        term = jnp.sum((t * t).reshape(BLK // 8, 8, t.shape[1]), axis=0)
        total = term if total is None else total + term
    for copy in range(squares_ref.shape[0]):
        squares_ref[copy] = total


def gather_kernel(got_ref, out_ref):
    total = jnp.sum(got_ref[...], axis=0)
    for copy in range(out_ref.shape[0]):
        out_ref[copy] = total


def scale_kernel(total_rows, t_ref, got_ref, out_ref):
    squares = jnp.sum(jnp.sum(got_ref[...], axis=0), axis=0, keepdims=True)
    out_ref[...] = t_ref[...] / jnp.sqrt(squares / total_rows + 1e-06)


def call(kernel, outs, operands, specs=None, flops=1e6, moved=1e6, scratch=()):
    return pl.pallas_call(
        kernel,
        out_shape=[jax.ShapeDtypeStruct(s, d) for s, d in outs],
        in_specs=specs or [VMEM] * len(operands),
        out_specs=[VMEM] * len(outs),
        scratch_shapes=scratch,
        compiler_params=pltpu.CompilerParams(vmem_limit_bytes=16 * 1024 * 1024),
        cost_estimate=cost(flops, moved),
    )(*operands)


def exchanged(pieces, axes):
    return lax.all_to_all(pieces, axes, split_axis=0, concat_axis=0, tiled=True)


def shards(vectors, near_blocks, leaf_basis, transfer, leaf_coupling, leaf_partners, parent_coupling, parent_partners, shifts):
    rows, cols = vectors.shape
    rank = leaf_basis.shape[1]
    blocks = near_blocks.shape[0]
    n_narrow, n_wide = lax.axis_size(NARROW), lax.axis_size(WIDE)
    chips = lax.axis_size("narrow_0")
    devices = n_narrow * n_wide
    half = cols // 2
    matrix = transfer[0]
    shift = shifts[None, :]
    up = [(i, i + 1) for i in range(devices - 1)]
    down = [(b, a) for a, b in up]
    swap = [(0, 1), (1, 0)]
    count = chips

    state = [((rows, cols), BF16), ((2, cols, rank), BF16), ((BLK, cols), BF16), ((BLK, cols), BF16)]

    leaf_flops = 2 * 2 * rows * rank * cols


    def away(far):
        there = [(2 * c, 2 * ((c + far) % chips)) for c in range(chips)]
        return there + [(2 * c + 1, 2 * ((c - far) % chips) + 1) for c in range(chips)]

    previous, t = None, vectors
    v, load, low, high = call(begin_kernel, state, (vectors, leaf_basis, matrix), flops=leaf_flops)
    for step in range(DEGREE):
        scale = 1.0 if step == 0 else 2.0
        partner = lax.ppermute(load, "narrow_1", swap)
        (pair,) = call(pair_kernel, [((3, cols, rank), BF16)], (load, partner))
        ring, crossed = [pair], []
        for s in range(1, chips // 2 + 1):
            start = 0 if s < 3 else 2
            ring.append(lax.ppermute(ring[start], NARROW, away(s - start)))
            if s < chips // 2:
                crossed.append(lax.ppermute(ring[-1], "narrow_1", swap))
        loads = ring + crossed
        low_in = lax.ppermute(high, ALL, up)
        high_in = lax.ppermute(low, ALL, down)
        operands = [near_blocks, v, low_in, high_in, t, shift] + ([] if previous is None else [previous])
        (value,) = call(
            functools.partial(near_kernel, previous is None),
            [((rows, cols), F32)],
            operands,
            flops=2 * 3 * blocks * BLK * BLK * cols,
        )
        (share,) = call(share_kernel, [((n_wide, half, rank), BF16)], loads)
        (far,) = call(
            functools.partial(sibling_kernel, count),
            [((cols, rank), F32)],
            (leaf_partners[0], *loads, leaf_coupling[0]),
            [SMEM] + [VMEM] * (count + 1),
            flops=6 * 2 * rank * rank * cols,
            scratch=[pltpu.VMEM((2 * count, cols, rank), BF16)],
        )
        gathered = exchanged(share, WIDE)
        (mine,) = call(
            parent_kernel,
            [((half, rank), BF16)],
            (parent_partners[0], gathered, parent_coupling[0]),
            [SMEM, VMEM, VMEM],
        )
        theirs = lax.ppermute(mine, "narrow_1", swap)
        operands = (value, far, mine, theirs, matrix, leaf_basis)
        previous = t
        if step < DEGREE - 1:
            t, v, load, low, high = call(
                functools.partial(step_kernel, scale), [((rows, cols), F32)] + state, operands, flops=2 * leaf_flops
            )
        else:
            out, squares = call(
                functools.partial(final_kernel, scale),
                [((rows, cols), F32), ((n_narrow, 8, cols), F32)],
                operands,
                flops=leaf_flops,
            )
    squares = exchanged(squares, NARROW)
    (squares,) = call(gather_kernel, [((n_wide, 8, cols), F32)], (squares,))
    squares = exchanged(squares, WIDE)
    (out,) = call(functools.partial(scale_kernel, rows * devices), [((rows, cols), F32)], (out, squares))
    return out


def solution(mesh):
    finer = Mesh(mesh.devices.reshape(4, 4, 8, 2), ALL)
    placed = (
        P(ALL, None),
        P(ALL, None, None, None),
        P(ALL, None),
        P(ALL, None, None),
        P(ALL, None, None, None),
        P(ALL, None),
        P(WIDE, None, None, None),
        P(WIDE, None),
        P(),
    )
    return jax.shard_map(shards, mesh=finer, in_specs=placed, out_specs=P(ALL, None), check_vma=False)
```

```python
import functools

import jax
import jax.numpy as jnp
from jax import lax
from jax.experimental import pallas as pl
from jax.experimental.pallas import tpu as pltpu
from jax.sharding import Mesh
from jax.sharding import PartitionSpec as P


BLK = 512
DEGREE = 3
ALL = ("wide_0", "wide_1", "narrow_0", "narrow_1")
NARROW = ("narrow_0", "narrow_1")
WIDE = ("wide_0", "wide_1")
F32 = jnp.float32
BF16 = jnp.bfloat16
VMEM = pl.BlockSpec(memory_space=pltpu.VMEM)
SMEM = pl.BlockSpec(memory_space=pltpu.SMEM)


def cost(flops, moved):
    return pl.CostEstimate(flops=int(flops), bytes_accessed=int(moved), transcendentals=0)


def dot_nn(a, b):
    return lax.dot_general(a, b, (((1,), (0,)), ((), ())), preferred_element_type=F32)


def dot_nt(a, b):
    return lax.dot_general(a, b, (((1,), (1,)), ((), ())), preferred_element_type=F32)


def block(b):
    return slice(b * BLK, (b + 1) * BLK)


def send(total, transfer_ref, load_ref):
    coeff = total.astype(BF16)
    load_ref[0] = coeff
    load_ref[1] = dot_nn(coeff, transfer_ref[...]).astype(BF16)


def begin_kernel(
    vec_hbm, basis_hbm, transfer_hbm, v_ref, load_ref, low_ref, high_ref, vec_ref, basis_ref, transfer_ref, sems
):
    blocks = vec_ref.shape[0] // BLK
    copies = []
    for b in range(blocks):
        copies.append(pltpu.make_async_copy(vec_hbm.at[block(b), :], vec_ref.at[block(b), :], sems.at[2 * b]))
        copies.append(pltpu.make_async_copy(basis_hbm.at[block(b), :], basis_ref.at[block(b), :], sems.at[2 * b + 1]))
    copies.append(pltpu.make_async_copy(transfer_hbm, transfer_ref, sems.at[2 * blocks]))
    for copy in copies:
        copy.start()
    total = None
    for b in range(blocks):
        copies[2 * b].wait()
        t = vec_ref[block(b), :]
        v = t.astype(BF16)
        v_ref[block(b), :] = v
        if b == 0:
            low_ref[...] = v
        if b == blocks - 1:
            high_ref[...] = v
        copies[2 * b + 1].wait()
        term = dot_nn(t.T.astype(BF16), basis_ref[block(b), :])
        total = term if total is None else total + term
    copies[-1].wait()
    send(total, transfer_ref, load_ref)


def near_kernel(first, blocks_ref, v_ref, low_ref, high_ref, t_ref, shift_ref, *rest):
    out_ref = rest[-1]
    blocks = blocks_ref.shape[0]
    for b in range(blocks):
        near = dot_nn(blocks_ref[b, 0], low_ref[...] if b == 0 else v_ref[block(b - 1), :])
        near = near + dot_nn(blocks_ref[b, 1], v_ref[block(b), :])
        near = near + dot_nn(blocks_ref[b, 2], high_ref[...] if b == blocks - 1 else v_ref[block(b + 1), :])
        value = near - shift_ref[...] * t_ref[block(b), :]
        if not first:
            value = 2.0 * value - rest[0][block(b), :]
        out_ref[block(b), :] = value


def share_kernel(*refs):
    loads, out_ref = refs[:-1], refs[-1]
    half = out_ref.shape[1]
    rows = pl.ds(pl.multiple_of(lax.axis_index("narrow_1") * half, half), half)
    total = loads[0][2, rows, :].astype(F32)
    for load_ref in loads[1:]:
        total = total + load_ref[2, rows, :].astype(F32)
    total = total.astype(BF16)
    for copy in range(out_ref.shape[0]):
        out_ref[copy] = total


def parent_kernel(partner_ref, got_ref, coupling_ref, out_ref):
    total = dot_nt(got_ref[partner_ref[0]], coupling_ref[0])
    for j in range(1, coupling_ref.shape[0]):
        total = total + dot_nt(got_ref[partner_ref[j]], coupling_ref[j])
    out_ref[...] = total.astype(BF16)


def pair_kernel(own_ref, other_ref, out_ref):
    out_ref[0] = own_ref[0]
    out_ref[1] = other_ref[0]
    out_ref[2] = (own_ref[1].astype(F32) + other_ref[1].astype(F32)).astype(BF16)


def sibling_kernel(count, partner_ref, *refs):
    loads, (coupling_ref, out_ref, held) = refs[:count], refs[count:]
    for k, load_ref in enumerate(loads):
        for slot in range(2):
            held[2 * k + slot] = load_ref[slot]
    chips = lax.axis_size("narrow_0")
    chip, core = lax.axis_index("narrow_0"), lax.axis_index("narrow_1")
    half = chips // 2
    total = None
    for j in range(coupling_ref.shape[0]):
        leaf = partner_ref[j]
        parity = lax.rem(leaf, 2)
        away = lax.rem(chip - leaf // 2 + chips, chips)
        own_ring = jnp.logical_or(away == 0, away == half)
        ring_core = jnp.where(own_ring, core, jnp.where(away < half, 0, 1))
        hops = jnp.where(away <= half, away, chips - away)
        at = jnp.where(ring_core == core, hops, half + hops)
        at = 2 * at + jnp.where(parity == ring_core, 0, 1)
        term = dot_nt(held[at], coupling_ref[j])
        total = term if total is None else total + term
    out_ref[...] = total


def far_of(far_ref, mine_ref, theirs_ref, transfer_ref):
    mine, theirs = dot_nt(mine_ref[...], transfer_ref[...]), dot_nt(theirs_ref[...], transfer_ref[...])
    first = lax.axis_index("narrow_1") == 0
    down = jnp.concatenate([jnp.where(first, mine, theirs), jnp.where(first, theirs, mine)], axis=0)
    return (far_ref[...] + down).T.astype(BF16)


def step_kernel(
    scale, part_ref, far_ref, mine_ref, theirs_ref, transfer_ref, basis_ref, t_ref, v_ref, load_ref, low_ref, high_ref
):
    blocks = part_ref.shape[0] // BLK
    far = far_of(far_ref, mine_ref, theirs_ref, transfer_ref)
    total = None
    for b in range(blocks):
        basis = basis_ref[block(b), :]
        t = part_ref[block(b), :] + scale * dot_nn(basis, far)
        t_ref[block(b), :] = t
        v = t.astype(BF16)
        v_ref[block(b), :] = v
        if b == 0:
            low_ref[...] = v
        if b == blocks - 1:
            high_ref[...] = v
        term = dot_nn(t.T.astype(BF16), basis)
        total = term if total is None else total + term
    send(total, transfer_ref, load_ref)


def final_kernel(scale, part_ref, far_ref, mine_ref, theirs_ref, transfer_ref, basis_ref, out_ref, squares_ref):
    far = far_of(far_ref, mine_ref, theirs_ref, transfer_ref)
    total = None
    for b in range(part_ref.shape[0] // BLK):
        t = part_ref[block(b), :] + scale * dot_nn(basis_ref[block(b), :], far)
        out_ref[block(b), :] = t
        term = jnp.sum((t * t).reshape(BLK // 8, 8, t.shape[1]), axis=0)
        total = term if total is None else total + term
    for copy in range(squares_ref.shape[0]):
        squares_ref[copy] = total


def gather_kernel(got_ref, out_ref):
    total = jnp.sum(got_ref[...], axis=0)
    for copy in range(out_ref.shape[0]):
        out_ref[copy] = total


def scale_kernel(total_rows, t_ref, got_ref, out_ref):
    squares = jnp.sum(jnp.sum(got_ref[...], axis=0), axis=0, keepdims=True)
    out_ref[...] = t_ref[...] / jnp.sqrt(squares / total_rows + 1e-06)


def call(kernel, outs, operands, specs=None, flops=1e6, moved=1e6, scratch=(), mib=16):
    return pl.pallas_call(
        kernel,
        out_shape=[jax.ShapeDtypeStruct(s, d) for s, d in outs],
        in_specs=specs or [VMEM] * len(operands),
        out_specs=[VMEM] * len(outs),
        scratch_shapes=scratch,
        compiler_params=pltpu.CompilerParams(vmem_limit_bytes=mib * 1024 * 1024),
        cost_estimate=cost(flops, moved),
    )(*operands)


def exchanged(pieces, axes):
    return lax.all_to_all(pieces, axes, split_axis=0, concat_axis=0, tiled=True)


def shards(vectors, near_blocks, leaf_basis, transfer, leaf_coupling, leaf_partners, parent_coupling, parent_partners, shifts):
    rows, cols = vectors.shape
    rank = leaf_basis.shape[1]
    blocks = near_blocks.shape[0]
    n_narrow, n_wide = lax.axis_size(NARROW), lax.axis_size(WIDE)
    chips = lax.axis_size("narrow_0")
    devices = n_narrow * n_wide
    half = cols // 2
    matrix = transfer[0]
    shift = shifts[None, :]
    up = [(i, i + 1) for i in range(devices - 1)]
    down = [(b, a) for a, b in up]
    swap = [(0, 1), (1, 0)]
    count = chips
    state = [((rows, cols), BF16), ((2, cols, rank), BF16), ((BLK, cols), BF16), ((BLK, cols), BF16)]
    leaf_flops = 2 * 2 * rows * rank * cols

    def away(far):
        there = [(2 * c, 2 * ((c + far) % chips)) for c in range(chips)]
        return there + [(2 * c + 1, 2 * ((c - far) % chips) + 1) for c in range(chips)]

    previous, t = None, vectors
    v, load, low, high = call(
        begin_kernel,
        state,
        (vectors, leaf_basis, matrix),
        [pl.BlockSpec(memory_space=pltpu.HBM)] * 3,
        flops=leaf_flops,
        mib=60,
        scratch=[
            pltpu.VMEM(vectors.shape, F32),
            pltpu.VMEM(leaf_basis.shape, BF16),
            pltpu.VMEM(matrix.shape, BF16),
            pltpu.SemaphoreType.DMA((2 * blocks + 1,)),
        ],
    )
    for step in range(DEGREE):
        scale = 1.0 if step == 0 else 2.0
        partner = lax.ppermute(load, "narrow_1", swap)
        (pair,) = call(pair_kernel, [((3, cols, rank), BF16)], (load, partner))
        ring, crossed = [pair], []
        for s in range(1, chips // 2 + 1):
            start = 0 if s < 3 else 2
            ring.append(lax.ppermute(ring[start], NARROW, away(s - start)))
            if s < chips // 2:
                crossed.append(lax.ppermute(ring[-1], "narrow_1", swap))
        loads = ring + crossed
        low_in = lax.ppermute(high, ALL, up)
        high_in = lax.ppermute(low, ALL, down)
        operands = [near_blocks, v, low_in, high_in, t, shift] + ([] if previous is None else [previous])
        (value,) = call(
            functools.partial(near_kernel, previous is None),
            [((rows, cols), F32)],
            operands,
            flops=2 * 3 * blocks * BLK * BLK * cols,
        )
        (share,) = call(share_kernel, [((n_wide, half, rank), BF16)], loads)
        (far,) = call(
            functools.partial(sibling_kernel, count),
            [((cols, rank), F32)],
            (leaf_partners[0], *loads, leaf_coupling[0]),
            [SMEM] + [VMEM] * (count + 1),
            flops=6 * 2 * rank * rank * cols,
            scratch=[pltpu.VMEM((2 * count, cols, rank), BF16)],
        )
        gathered = exchanged(share, WIDE)
        (mine,) = call(
            parent_kernel,
            [((half, rank), BF16)],
            (parent_partners[0], gathered, parent_coupling[0]),
            [SMEM, VMEM, VMEM],
        )
        theirs = lax.ppermute(mine, "narrow_1", swap)
        operands = (value, far, mine, theirs, matrix, leaf_basis)
        previous = t
        if step < DEGREE - 1:
            t, v, load, low, high = call(
                functools.partial(step_kernel, scale), [((rows, cols), F32)] + state, operands, flops=2 * leaf_flops
            )
        else:
            out, squares = call(
                functools.partial(final_kernel, scale),
                [((rows, cols), F32), ((n_narrow, 8, cols), F32)],
                operands,
                flops=leaf_flops,
            )
    squares = exchanged(squares, NARROW)
    (squares,) = call(gather_kernel, [((n_wide, 8, cols), F32)], (squares,))
    squares = exchanged(squares, WIDE)
    (out,) = call(functools.partial(scale_kernel, rows * devices), [((rows, cols), F32)], (out, squares))
    return out


def solution(mesh):
    finer = Mesh(mesh.devices.reshape(4, 4, 8, 2), ALL)
    placed = (
        P(ALL, None),
        P(ALL, None, None, None),
        P(ALL, None),
        P(ALL, None, None),
        P(ALL, None, None, None),
        P(ALL, None),
        P(WIDE, None, None, None),
        P(WIDE, None),
        P(),
    )
    return jax.shard_map(shards, mesh=finer, in_specs=placed, out_specs=P(ALL, None), check_vma=False)
```
